32 devices in a mesh: src: 4 (over x, core), gauge: 8 (over z, y).
Axes of the slice: x: 2, y: 2, z: 4, core: 2. Of those that a mesh axis runs over, the one named last changes fastest.
Arguments:
- green: bfloat16 [128, 512, 4096], P('gauge', None, 'src'), may hold values from -0.234375 to 0.234375
- observed: float32 [128, 128, 512], P(None, 'gauge'), may hold values from -8 to 8
- gauge_mask: int32 [128], P('gauge'), may hold values 0 or 1
- source_mask: int32 [4096], P('src'), may hold values 0 or 1
Outputs:
- slip: float32 [128, 4096], P(None, 'src')
- residual: float32 [128, 128, 512], P(None, 'gauge')
The draws below stay inside these ranges and needn't reach their ends.
All inputs are finite; a program needn't handle non-finite values. No bound on the sum of `gauge_mask` or of `source_mask` on one device may be relied on, other than what follows from the above.
Results may differ from the reference program's by a relative error of at most 0.023.
Values may be sent and summed in bfloat16 or wider, within the bound.
A program may use at most 64 MiB of HBM per device.

```python
import jax
import jax.numpy as jnp
from jax import lax

S = 4096
T_SIZE = 512
K = 128
ITERS = 3
GAUGES = 128
N_SRC = 4


def shared_green(key):
    place = jnp.arange(GAUGES, dtype=jnp.float32) / max(GAUGES - 1, 1)
    value_key = jax.random.fold_in(key, 11)
    column_key = jax.random.fold_in(key, 12)
    values = jnp.clip(jax.random.normal(value_key, (GAUGES, T_SIZE, S), jnp.float32), -6.0, 6.0)
    rising = 10.0 ** (0.5 * place)
    columns = jnp.exp(jax.random.uniform(column_key, (S,), jnp.float32, -2.302585, 0.0))
    scaled = values * (rising * (GAUGES * T_SIZE) ** (-0.5))[:, None, None] * columns[None, None, :]
    return (scaled.astype(jnp.bfloat16), columns)


def draw_green(key, part):
    green, columns = shared_green(key)
    return green


def draw_observed(key, part):
    green, columns = shared_green(key)
    slip_key = jax.random.fold_in(key, 13)
    noise_key = jax.random.fold_in(key, 14)
    amplitude = jax.random.normal(slip_key, (K, S), jnp.float32) / columns[None, :]
    signal = lax.dot_general(amplitude.astype(jnp.bfloat16), green, (((1,), (2,)), ((), ())), preferred_element_type=jnp.float32)
    signal = signal * lax.rsqrt(jnp.mean(signal * signal) + 1e-12)
    noise = jax.random.normal(noise_key, (K, GAUGES, T_SIZE), jnp.float32)
    return jnp.clip(signal + 0.05 * noise, -8.0, 8.0)


def set_ends(values, own_key, least, top_value):
    spot = [jax.random.randint(jax.random.fold_in(own_key, axis), (), 0, length) for axis, length in enumerate(values.shape)]
    widest = values.shape.index(max(values.shape))
    beside = spot[:widest] + [(spot[widest] + 1) % values.shape[widest]] + spot[widest + 1:]
    return values.at[tuple(spot)].set(least).at[tuple(beside)].set(top_value)


def setup_inputs(seed: int = 0) -> dict:
    streams_of = jax.random.split(jax.random.key(seed), 5)
    green = draw_green(jax.random.fold_in(streams_of[4], 71), 0)
    observed = draw_observed(jax.random.fold_in(streams_of[4], 71), 0)
    gauge_mask = set_ends((jax.random.randint(streams_of[2], (GAUGES,), 0, 8) < 7).astype(jnp.int32), jax.random.fold_in(streams_of[2], 1), 0, 1)
    source_mask = set_ends((jax.random.randint(streams_of[3], (S,), 0, 4) < 3).astype(jnp.int32), jax.random.fold_in(streams_of[3], 1), 0, 1)
    return {"green": green, "observed": observed, "gauge_mask": gauge_mask, "source_mask": source_mask}


def forward(green, vector, wg):
    width = green.shape[2] // N_SRC
    total = jnp.zeros((vector.shape[0], green.shape[0], green.shape[1]), jnp.float32)
    for block in range(N_SRC):
        piece = green[:, :, block * width:(block + 1) * width]
        rows = vector[:, block * width:(block + 1) * width]
        part = lax.dot_general(rows, piece, (((1,), (2,)), ((), ())), preferred_element_type=jnp.float32)
        rounded = lax.optimization_barrier(part.astype(jnp.bfloat16))
        total = total + rounded.astype(jnp.float32)
    return wg * total


def adjoint(green, wave, ps):
    out = lax.dot_general(wave, green, (((1, 2), (0, 1)), ((), ())), preferred_element_type=jnp.float32)
    return ps * out


def reference(green, observed, gauge_mask, source_mask):
    wg = gauge_mask.astype(jnp.float32)[None, :, None]
    ps = source_mask.astype(jnp.float32)[None, :]
    residual = wg * observed
    slip = jnp.zeros((observed.shape[0], green.shape[2]), jnp.float32)
    grad = adjoint(green, residual.astype(jnp.bfloat16), ps)
    direction = grad
    gamma = jnp.sum(grad * grad, axis=1)
    for step in range(ITERS):
        predicted = forward(green, direction.astype(jnp.bfloat16), wg)
        curvature = jnp.sum(predicted * predicted, axis=(1, 2))
        alpha = gamma / curvature
        slip = slip + alpha[:, None] * direction
        residual = residual - alpha[:, None, None] * predicted
        if step + 1 < ITERS:
            grad = adjoint(green, residual.astype(jnp.bfloat16), ps)
            fresh = jnp.sum(grad * grad, axis=1)
            direction = grad + (fresh / gamma)[:, None] * direction
            gamma = fresh
    return slip, residual
```

```python
import functools

import jax
import jax.numpy as jnp
from jax import lax
from jax.experimental import pallas as pl
from jax.experimental.pallas import tpu as pltpu
from jax.sharding import PartitionSpec as P

ITERS = 3
GROUPS = 2
PAIR = 2
LAG = 2
LANES = 128
MESH = pl.DeviceIdType.MESH
F32 = jnp.float32
BF16 = jnp.bfloat16


def cg_kernel(
    peers, src_size, gpc,
    green_hbm, obs_ref, wg_ref, ps_ref,
    slip_ref, res_ref,
    green, part, r1, xs, xr, u, v, grad, gbf, dirn, vdir, csum, coef,
    gs, gr, ag, aq, cr, ca, cq, gm, gmr,
    green_sem, s1_send, s1_recv, x_send, x_recv, u_send, u_recv,
    rs_send, rs_recv, ag_send, ag_recv, cs_send, cs_recv, ca_send, ca_recv, gm_send, gm_recv,
):
    gauges, times, width = green.shape
    events = v.shape[0]
    eg = events // GROUPS
    half = eg // 2
    own = eg // peers
    chunks = gauges // gpc
    src = lax.axis_index("src")
    me = lax.axis_index("gauge")
    core = src % PAIR
    chip = src // PAIR
    sib = chip * PAIR + (1 - core)
    across = (1 - chip) * PAIR + core

    def green_copy(g):
        return pltpu.make_async_copy(green_hbm.at[g], green.at[g], green_sem.at[g])

    def start_green(g, _):
        green_copy(g).start()
        return 0

    lax.fori_loop(0, gauges, start_green, 0)

    barrier = pltpu.get_barrier_semaphore()
    for d in range(1, peers):
        pl.semaphore_signal(barrier, inc=1, device_id={"gauge": (me + d) % peers}, device_id_type=MESH)
    for d in range(1, src_size):
        pl.semaphore_signal(barrier, inc=1, device_id={"src": (src + d) % src_size}, device_id_type=MESH)
    pl.semaphore_wait(barrier, peers + src_size - 2)

    def rows(q):
        return slice(q * eg, (q + 1) * eg)

    def mine(q):
        return pl.ds(pl.multiple_of(q * eg + core * half, half), half)

    def theirs(q):
        return pl.ds(pl.multiple_of(q * eg + (1 - core) * half, half), half)

    def packed(q):
        return slice(q * half, (q + 1) * half)

    def span(c):
        return pl.ds(c * gpc, gpc)

    my_cols = pl.ds(pl.multiple_of(me * LANES, LANES), LANES)

    def rcopy(src_ref, dst_ref, send, recv, to):
        return pltpu.make_async_remote_copy(
            src_ref=src_ref, dst_ref=dst_ref, send_sem=send, recv_sem=recv,
            device_id=to, device_id_type=MESH,
        )

    def s1_copy(it, q, c):
        return rcopy(part.at[it, span(c), theirs(q)], r1.at[it, span(c), packed(q)],
                     s1_send.at[it, q, c], s1_recv.at[it, q, c], {"src": sib})

    def x_copy(it, q, c):
        return rcopy(xs.at[it, span(c), packed(q)], xr.at[it, span(c), packed(q)],
                     x_send.at[it, q, c], x_recv.at[it, q, c], {"src": across})

    def u_copy(it, q, c):
        return rcopy(u.at[it, span(c), mine(q)], u.at[it, span(c), mine(q)],
                     u_send.at[it, q, c], u_recv.at[it, q, c], {"src": sib})

    def u_arrive(it, q, c):
        return rcopy(u.at[it, span(c), theirs(q)], u.at[it, span(c), theirs(q)],
                     u_send.at[it, q, c], u_recv.at[it, q, c], {"src": sib})

    def rs_copy(k, q, d):
        p = (me + d) % peers
        cols = pl.ds(pl.multiple_of(p * LANES, LANES), LANES)
        return rcopy(gs.at[k, q, :, cols], gr.at[k, q, d - 1],
                     rs_send.at[k, q, d - 1], rs_recv.at[k, q, d - 1], {"gauge": p})

    def ag_copy(k, q, d):
        p = (me + d) % peers
        return rcopy(ag.at[k, q], aq.at[k, q, :, my_cols],
                     ag_send.at[k, q, d - 1], ag_recv.at[k, q, d - 1], {"gauge": p})

    def ag_arrive(k, q, d):
        p = (me + peers - d) % peers
        cols = pl.ds(pl.multiple_of(p * LANES, LANES), LANES)
        return rcopy(ag.at[k, q], aq.at[k, q, :, cols],
                     ag_send.at[k, q, d - 1], ag_recv.at[k, q, d - 1], {"gauge": p})

    def own_rows(p):
        return pl.ds(pl.multiple_of(p * own, own), own)

    def cs_copy(it, q, d):
        p = (me + d) % peers
        return rcopy(csum.at[it, q, own_rows(p)], cr.at[it, q, d - 1],
                     cs_send.at[it, q, d - 1], cs_recv.at[it, q, d - 1], {"gauge": p})

    def ca_copy(it, q, d):
        p = (me + d) % peers
        return rcopy(ca.at[it, q], cq.at[it, q, own_rows(me)],
                     ca_send.at[it, q, d - 1], ca_recv.at[it, q, d - 1], {"gauge": p})

    def ca_arrive(it, q, d):
        p = (me + peers - d) % peers
        return rcopy(ca.at[it, q], cq.at[it, q, own_rows(p)],
                     ca_send.at[it, q, d - 1], ca_recv.at[it, q, d - 1], {"gauge": p})

    def gm_copy(it, q, d):
        return rcopy(gm.at[it, q], gmr.at[it, q, d - 1],
                     gm_send.at[it, q, d - 1], gm_recv.at[it, q, d - 1],
                     {"src": (src + d) % src_size})

    hops = range(1, peers)

    def rs_start(k, q, with_v, it):
        if with_v:
            gs[k, q] = v[rows(q), :].astype(BF16)
        if it is not None:
            csum[it, q] = jnp.broadcast_to(
                jnp.sum(csum[it, q], axis=1, keepdims=True), (eg, LANES))
        for d in hops:
            if it is not None:
                cs_copy(it, q, d).start()
            if with_v:
                rs_copy(k, q, d).start()

    def ag_start(k, q, with_v, it):
        if it is not None:
            total = csum[it, q, own_rows(me)]
            for d in hops:
                cs_copy(it, q, d).wait_recv()
                total = total + cr[it, q, d - 1]
            ca[it, q] = total
            for d in hops:
                ca_copy(it, q, d).start()
            cq[it, q, own_rows(me)] = total
        if with_v:
            total = v[rows(q), my_cols]
            for d in hops:
                rs_copy(k, q, d).wait_recv()
                total = total + gr[k, q, d - 1].astype(F32)
            ag[k, q] = total.astype(BF16)
            for d in hops:
                ag_copy(k, q, d).start()
            aq[k, q, :, my_cols] = total.astype(BF16)

    def ag_wait(k, q, with_v, it):
        if it is not None:
            for d in hops:
                ca_arrive(it, q, d).wait_recv()
        if with_v:
            for d in hops:
                ag_arrive(k, q, d).wait_recv()

    def gamma_wait(it, q):
        total = gm[it, q]
        for d in range(1, src_size):
            gm_copy(it, q, d).wait_recv()
            total = total + gmr[it, q, d - 1]
        coef[0, it, q] = total
        if it > 0:
            coef[1, it, q] = total / coef[0, it - 1, q]

    def alpha_of(it, q):
        return coef[0, it, q] / cq[it, q]

    def close(it, q):
        a = alpha_of(it, q)
        coef[2, it, q] = a
        r = rows(q)
        if it == 0:
            dirn[r, :] = grad[r, :]
            slip_ref[r, :] = a[:, :1] * grad[r, :]
        else:
            d = grad[r, :] + coef[1, it, q][:, :1] * dirn[r, :]
            dirn[r, :] = d
            slip_ref[r, :] = slip_ref[r, :] + a[:, :1] * d

    def open_grad(it, q):
        r = rows(q)
        ps = ps_ref[...].astype(F32)
        full = aq[it, q].astype(F32)
        if it == 0:
            g = ps * full
        else:
            prev = it - 1
            if prev == 0:
                q_dir = full
            else:
                q_dir = full + coef[1, prev, q][:, :1] * vdir[r, :]
            vdir[r, :] = q_dir
            g = grad[r, :] - coef[2, prev, q][:, :1] * (ps * q_dir)
        grad[r, :] = g
        gbf[r, :] = g.astype(BF16)
        gm[it, q] = jnp.broadcast_to(jnp.sum(g * g, axis=1, keepdims=True), (eg, LANES))
        for d in range(1, src_size):
            gm_copy(it, q, d).start()

    def f1(it, q, begin, end):
        def step(c, _):
            @pl.when(c < chunks)
            def _():
                for i in range(gpc):
                    g = c * gpc + i
                    part[it, g, rows(q), :] = lax.dot_general(
                        gbf[rows(q), :], green[g], (((1,), (1,)), ((), ())),
                        preferred_element_type=F32).astype(BF16)
                s1_copy(it, q, c).start()

            @pl.when(c >= LAG)
            def _():
                b = c - LAG
                s1_copy(it, q, b).wait_recv()
                xs[it, span(b), packed(q)] = (
                    part[it, span(b), mine(q)].astype(F32)
                    + r1[it, span(b), packed(q)].astype(F32)).astype(BF16)
                x_copy(it, q, b).start()
            return 0

        lax.fori_loop(begin, end, step, 0)

    def f2(it, q, begin, end):
        def step(c, _):
            @pl.when(c < chunks)
            def _():
                x_copy(it, q, c).wait_recv()
                for i in range(gpc):
                    g = c * gpc + i
                    w = wg_ref[g].astype(F32)
                    u[it, g, mine(q), :] = (w * (
                        xs[it, g, packed(q)].astype(F32)
                        + xr[it, g, packed(q)].astype(F32))).astype(BF16)
                u_copy(it, q, c).start()

            @pl.when(c >= LAG)
            def _():
                b = c - LAG
                u_arrive(it, q, b).wait_recv()
                for i in range(gpc):
                    g = b * gpc + i
                    ug = u[it, g, rows(q), :]
                    if it + 1 < ITERS:
                        v[rows(q), :] += jnp.dot(ug, green[g], preferred_element_type=F32)
                    p = u[0, g, rows(q), :].astype(F32)
                    for k in range(1, it + 1):
                        p = u[k, g, rows(q), :].astype(F32) + coef[1, k, q][:, :1] * p
                    p = p * p
                    acc = csum[it, q]
                    for t in range(times // LANES):
                        acc = acc + p[:, t * LANES:(t + 1) * LANES]
                    csum[it, q] = acc
            return 0

        lax.fori_loop(begin, end, step, 0)

    v[...] = jnp.zeros_like(v)
    csum[...] = jnp.zeros_like(csum)

    def first(g, _):
        w = wg_ref[g].astype(F32)
        r0 = (w * obs_ref[:, g, :]).astype(BF16)
        green_copy(g).wait()
        v[...] += jnp.dot(r0, green[g], preferred_element_type=F32)
        return 0

    lax.fori_loop(0, gauges, first, 0)

    for q in range(GROUPS):
        rs_start(0, q, True, None)
    ag_start(0, 0, True, None)

    mid = chunks // 2
    last = chunks + LAG
    for it in range(ITERS):
        prev = it - 1 if it > 0 else None
        for q in range(GROUPS):
            ag_wait(it, q, True, prev)
            if prev is not None:
                close(prev, q)
            open_grad(it, q)
            if q + 1 < GROUPS:
                f1(it, q, 0, mid)
                ag_start(it, q + 1, True, prev)
                f1(it, q, mid, last)
            else:
                f1(it, q, 0, last)
        with_v = it + 1 < ITERS
        v[...] = jnp.zeros_like(v)
        for q in range(GROUPS):
            gamma_wait(it, q)
            if q > 0:
                f2(it, q, 0, mid)
                ag_start(it + 1, q - 1, with_v, it)
                f2(it, q, mid, last)
            else:
                f2(it, q, 0, last)
            rs_start(it + 1, q, with_v, it)
    ag_start(ITERS, GROUPS - 1, False, ITERS - 1)
    weights = []
    for q in range(GROUPS):
        ag_wait(ITERS, q, False, ITERS - 1)
        close(ITERS - 1, q)
        total = coef[2, ITERS - 1, q]
        ws = [total]
        for k in range(ITERS - 2, -1, -1):
            total = coef[2, k, q] + coef[1, k + 1, q] * total
            ws.insert(0, total)
        for k in range(ITERS):
            coef[0, k, q] = ws[k]

    def finish(g, _):
        w = wg_ref[g].astype(F32)
        for q in range(GROUPS):
            out = w * obs_ref[rows(q), g, :]
            for k in range(ITERS):
                out = out - coef[0, k, q][:, :1] * u[k, g, rows(q), :].astype(F32)
            res_ref[rows(q), g, :] = out
        return 0

    lax.fori_loop(0, gauges, finish, 0)

    def drain(c, _):
        for it in range(ITERS):
            for q in range(GROUPS):
                s1_copy(it, q, c).wait_send()
                x_copy(it, q, c).wait_send()
                u_copy(it, q, c).wait_send()
        return 0

    lax.fori_loop(0, chunks, drain, 0)
    for it in range(ITERS):
        for q in range(GROUPS):
            for d in hops:
                rs_copy(it, q, d).wait_send()
                ag_copy(it, q, d).wait_send()
                cs_copy(it, q, d).wait_send()
                ca_copy(it, q, d).wait_send()
            for d in range(1, src_size):
                gm_copy(it, q, d).wait_send()


def fused(peers, src_size, green, observed, gauge_mask, source_mask):
    gauges, times, width = green.shape
    events = observed.shape[0]
    eg = events // GROUPS
    own = eg // peers
    gpc = 2
    chunks = gauges // gpc
    vm = pltpu.VMEM
    dma = pltpu.SemaphoreType.DMA
    n = peers - 1
    m = src_size - 1
    scratch = [
        vm((gauges, times, width), BF16),
        vm((ITERS, gauges, events, times), BF16),
        vm((ITERS, gauges, events // 2, times), BF16),
        vm((ITERS, gauges, events // 2, times), BF16),
        vm((ITERS, gauges, events // 2, times), BF16),
        vm((ITERS, gauges, events, times), BF16),
        vm((events, width), F32),
        vm((events, width), F32),
        vm((events, width), BF16),
        vm((events, width), F32),
        vm((events, width), F32),
        vm((ITERS, GROUPS, eg, LANES), F32),
        vm((3, ITERS, GROUPS, eg, LANES), F32),
        vm((ITERS, GROUPS, eg, width), BF16),
        vm((ITERS, GROUPS, n, eg, LANES), BF16),
        vm((ITERS, GROUPS, eg, LANES), BF16),
        vm((ITERS, GROUPS, eg, width), BF16),
        vm((ITERS, GROUPS, n, own, LANES), F32),
        vm((ITERS, GROUPS, own, LANES), F32),
        vm((ITERS, GROUPS, eg, LANES), F32),
        vm((ITERS, GROUPS, eg, LANES), F32),
        vm((ITERS, GROUPS, m, eg, LANES), F32),
        dma((gauges,)),
    ] + [dma((ITERS, GROUPS, chunks))] * 6 + [dma((ITERS, GROUPS, n))] * 8 + [dma((ITERS, GROUPS, m))] * 2
    slip, res = pl.pallas_call(
        functools.partial(cg_kernel, peers, src_size, gpc),
        out_shape=(
            jax.ShapeDtypeStruct((events, width), F32),
            jax.ShapeDtypeStruct((events, gauges, times), F32),
        ),
        in_specs=[
            pl.BlockSpec(memory_space=pl.ANY),
            pl.BlockSpec(memory_space=pltpu.VMEM),
            pl.BlockSpec(memory_space=pltpu.SMEM),
            pl.BlockSpec(memory_space=pltpu.VMEM),
        ],
        out_specs=[pl.BlockSpec(memory_space=pltpu.VMEM)] * 2,
        scratch_shapes=scratch,
        compiler_params=pltpu.CompilerParams(
            collective_id=0, has_side_effects=True, vmem_limit_bytes=67043328),
    )(green, observed, gauge_mask, source_mask.reshape(1, width))
    return slip, res


def project(vector, green):
    return lax.dot_general(
        vector, green, (((1,), (2,)), ((), ())), preferred_element_type=F32)


def gradient(green, wave, ps_local):
    part = lax.dot_general(
        wave.astype(BF16), green, (((1, 2), (0, 1)), ((), ())), preferred_element_type=F32)
    grad = ps_local * lax.psum(part.astype(BF16), "gauge").astype(F32)
    gamma = lax.psum(jnp.sum(grad * grad, axis=1), "src")
    return (grad, gamma)


def general(green, observed, gauge_mask, source_mask):
    wg = gauge_mask.astype(F32)[None, :, None]
    ps_local = source_mask.astype(F32)[None, :]
    residual = wg * observed
    events = observed.shape[0]
    slip = jnp.zeros((events, green.shape[2]), F32)
    grad, gamma = gradient(green, residual, ps_local)
    direction = grad
    for step in range(ITERS):
        rows = events // lax.axis_size("src")
        offset = lax.axis_index("src") * rows
        predicted = wg * lax.psum_scatter(
            project(direction.astype(BF16), green).astype(BF16),
            "src", scatter_dimension=0, tiled=True).astype(F32)
        curvature = lax.psum(jnp.sum(predicted * predicted, axis=(1, 2)), "gauge")
        alpha_rows = lax.dynamic_slice_in_dim(gamma, offset, rows, 0) / curvature
        kept = (lax.dynamic_slice_in_dim(residual, offset, rows, 0)
                - alpha_rows[:, None, None] * predicted)
        residual = lax.all_gather(kept.astype(BF16), "src", axis=0, tiled=True).astype(F32)
        alpha = lax.all_gather(alpha_rows.astype(BF16), "src", axis=0, tiled=True).astype(F32)
        slip = slip + alpha[:, None] * direction
        if step + 1 < ITERS:
            grad, fresh = gradient(green, residual, ps_local)
            direction = grad + (fresh / gamma)[:, None] * direction
            gamma = fresh
    return (slip, residual)


def per_device(peers, src_size, green, observed, gauge_mask, source_mask):
    events, gauges, times = observed.shape
    fits = (
        src_size == 2 * PAIR
        and green.shape[2] == peers * LANES
        and gauges % 4 == 0
        and gauges % 8 == 0
        and events % (GROUPS * 8 * peers) == 0
        and events % (GROUPS * 32) == 0
        and times % LANES == 0
    )
    if fits:
        return fused(peers, src_size, green, observed, gauge_mask, source_mask)
    return general(green, observed, gauge_mask, source_mask)


def solution(mesh):
    return jax.shard_map(
        functools.partial(per_device, mesh.shape["gauge"], mesh.shape["src"]),
        mesh=mesh,
        in_specs=(P("gauge", None, "src"), P(None, "gauge", None), P("gauge"), P("src")),
        out_specs=(P(None, "src"), P(None, "gauge", None)),
        check_vma=False,
    )
```
